256 devices in a mesh: dp: 8 (over x, z_lo), section: 8 (over z_hi, core), tensor: 4 (over y).
Axes of the slice: x: 4, y: 4, z: 8 (z_hi: 4, z_lo: 2; z = z_hi * 2 + z_lo), core: 2. Of those that a mesh axis runs over, the one named last changes fastest.
Arguments:
- cotangent: bfloat16 [2, 64, 6144], P(None, 'tensor', 'dp'), may hold values from -6 to 6
- inputs: bfloat16 [8, 2, 64, 6144], P('section', None, 'tensor', 'dp'), may hold values from -6 to 6
- queries: bfloat16 [8, 2, 64, 6144], P('section', None, None, 'tensor'), may hold values from -256 to 256
- keys: bfloat16 [8, 2, 64, 6144], P('section', None, None, 'tensor'), may hold values from -8 to 8
- context: bfloat16 [8, 2, 64, 6144], P('section', None, None, 'tensor'), may hold values from -6 to 6
- value_weight: bfloat16 [8, 6144, 6144], P('section', 'dp', 'tensor'), may hold values from -0.078125 to 0.078125
- out_weight: bfloat16 [8, 6144, 6144], P('section', 'tensor', 'dp'), may hold values from -0.078125 to 0.078125
Outputs:
- section_grads: bfloat16 [8, 2, 64, 6144], P('section', None, 'tensor', 'dp')
- value_weight_grad: bfloat16 [8, 6144, 6144], P('section', 'dp', 'tensor')
- out_weight_grad: bfloat16 [8, 6144, 6144], P('section', 'tensor', 'dp')
The draws below stay inside these ranges and needn't reach their ends.
All inputs are finite; a program needn't handle non-finite values.
Results may differ from the reference program's by a relative error of at most 0.018.
Values may be sent and summed in bfloat16 or wider, within the bound.
A program may use at most 64 MiB of HBM per device.

```python
import jax
import jax.numpy as jnp
from jax import lax

D = 6144
HEAD_DIM = 128
SEQ = 64
MICRO = 2
LAYERS = 8


def paired_draw(key):
    base = jax.random.fold_in(key, 7)
    key_query, key_key = jax.random.split(base, 2)
    shape = (LAYERS, MICRO, SEQ, D)
    query_all = jnp.clip(jax.random.normal(key_query, shape, jnp.float32), -5.0, 5.0)
    key_all = jnp.clip(jax.random.normal(key_key, shape, jnp.float32), -5.0, 5.0)
    return (query_all, key_all)


def draw_queries(key, part):
    return paired_draw(key)[0].astype(jnp.bfloat16)


def draw_keys(key, part):
    return paired_draw(key)[1].astype(jnp.bfloat16)


def level_of(key, dims, shards, least, largest):
    loudness = 1.0
    for position, parts in shards:
        steps = jax.random.uniform(jax.random.fold_in(jax.random.fold_in(key, 6), position), (parts,), jnp.float32, least / len(shards), largest / len(shards))
        loudness = loudness * jnp.repeat(jnp.exp(steps), dims[position] // parts).reshape((-1,) + (1,) * (len(dims) - 1 - position))
    return loudness


def gaussian(rng, dims, scale, bound, shards=(), dtype=jnp.bfloat16):
    values = jax.random.normal(rng, dims, jnp.float32) * scale
    if len(shards) > 0:
        values = level_of(rng, dims, shards, -0.22, 0.18) * values
    return jnp.clip(values, min=-bound, max=bound).astype(dtype)


def setup_inputs(seed: int = 0) -> dict:
    key_of = jax.random.split(jax.random.key(seed), 8)
    cotangent = gaussian(key_of[0], (MICRO, SEQ, D), 1.0, 6.0, ((1, 4), (2, 8)))
    inputs = gaussian(key_of[1], (LAYERS, MICRO, SEQ, D), 1.0, 6.0, ((0, 8), (2, 4), (3, 8)))
    queries = draw_queries(jax.random.fold_in(key_of[7], 71), 0)
    keys = draw_keys(jax.random.fold_in(key_of[7], 71), 0)
    context = gaussian(key_of[4], (LAYERS, MICRO, SEQ, D), 1.0, 6.0, ((0, 8), (3, 4)))
    value_weight = gaussian(key_of[5], (LAYERS, D, D), D ** -0.5, 0.078125, ((0, 8), (1, 8), (2, 4)))
    out_weight = gaussian(key_of[6], (LAYERS, D, D), D ** -0.5, 0.078125, ((0, 8), (1, 4), (2, 8)))
    return {"cotangent": cotangent, "inputs": inputs, "queries": queries, "keys": keys, "context": context, "value_weight": value_weight, "out_weight": out_weight}


def attention_probs(query_layer, key_layer):
    micro_count, seq_len, width = query_layer.shape
    head_count = width // HEAD_DIM
    query_heads = query_layer.astype(jnp.float32).reshape(micro_count, seq_len, head_count, HEAD_DIM)
    key_heads = key_layer.astype(jnp.float32).reshape(micro_count, seq_len, head_count, HEAD_DIM)
    scores = jnp.einsum('mihd,mjhd->mhij', query_heads, key_heads) / jnp.sqrt(jnp.float32(HEAD_DIM))
    rows = jnp.arange(seq_len)
    causal = rows[:, None] >= rows[None, :]
    scores = jnp.where(causal[None, None], scores, jnp.float32(-1e+30))
    highest = lax.optimization_barrier(jnp.max(scores, axis=-1, keepdims=True))
    expo = jnp.exp(scores - highest)
    return (expo / lax.optimization_barrier(jnp.sum(expo, axis=-1, keepdims=True))).astype(jnp.bfloat16)

def reference(cotangent, inputs, queries, keys, context, value_weight, out_weight):
    micro_count, seq_len, width = cotangent.shape
    head_count = width // HEAD_DIM
    upper = cotangent
    grads_list = []
    value_list = []
    out_list = []
    for layer in range(LAYERS - 1, -1, -1):
        upper_flat = upper.reshape(micro_count * seq_len, width)
        ctx_grad = jnp.dot(upper_flat.astype(jnp.float32), out_weight[layer].T.astype(jnp.float32), preferred_element_type=jnp.float32).astype(jnp.bfloat16)
        attention = attention_probs(queries[layer], keys[layer])
        ctx_heads = ctx_grad.reshape(micro_count, seq_len, head_count, HEAD_DIM).astype(jnp.float32)
        value_grad = jnp.einsum('mhij,mihd->mjhd', attention.astype(jnp.float32), ctx_heads)
        value_grad = value_grad.reshape(micro_count * seq_len, width).astype(jnp.bfloat16)
        branch = jnp.dot(value_grad.astype(jnp.float32), value_weight[layer].T.astype(jnp.float32), preferred_element_type=jnp.float32)
        lower = (upper_flat.astype(jnp.float32) + branch).astype(jnp.bfloat16)
        context_flat = context[layer].reshape(micro_count * seq_len, width)
        out_grad = jnp.dot(context_flat.T.astype(jnp.float32), upper_flat.astype(jnp.float32), preferred_element_type=jnp.float32).astype(jnp.bfloat16)
        input_flat = inputs[layer].reshape(micro_count * seq_len, width)
        value_wgrad = jnp.dot(input_flat.T.astype(jnp.float32), value_grad.astype(jnp.float32), preferred_element_type=jnp.float32).astype(jnp.bfloat16)
        upper = lower.reshape(micro_count, seq_len, width)
        grads_list.append(upper)
        value_list.append(value_wgrad)
        out_list.append(out_grad)
    grads_list = grads_list[::-1]
    value_list = value_list[::-1]
    out_list = out_list[::-1]
    return (jnp.stack(grads_list), jnp.stack(value_list), jnp.stack(out_list))
```

```python
import functools

import jax
import jax.numpy as jnp
from jax import lax
from jax.experimental import pallas as pl
from jax.experimental.pallas import tpu as pltpu
from jax.sharding import PartitionSpec as P

HEAD_DIM = 128
CTX_ROWS = 256
MESH = pl.DeviceIdType.MESH
F32 = jnp.float32
BF16 = jnp.bfloat16


def kernel(
    tokens,
    sections,
    cot, inp, q_hbm, k_hbm, wo_hbm, wv_hbm,
    grad_out, uin_out, vg_out, xin_out,
    wo, wv, q, k, att, cotg, xg, u, csend, crecv, acc, ysend, yrecv, ufin, turned,
    load_sem, own_sem, cs_sem, cr_sem, ys_sem, yr_sem, fs_sem, fr_sem, ag_sem, agr_sem, xs_sem, xr_sem,
):
    head_cols, width = wo.shape
    micro, part, _ = cot.shape
    seq = tokens // micro
    dp = lax.axis_index("dp")
    sec = lax.axis_index("section")
    ten = lax.axis_index("tensor")
    x, z = dp // 2, dp % 2
    dp_peers = ({"dp": x * 2 + (1 - z)}, {"dp": (x + 1 - 2 * (x % 2)) * 2 + z}, {"dp": (3 - x) * 2 + z})
    y_peers = ({"tensor": ten + 1 - 2 * (ten % 2)}, {"tensor": 3 - ten})
    y_all = [{"tensor": (ten + i) % 4} for i in (1, 2, 3)]
    above = {"section": jnp.minimum(sec + 1, sections - 1)}
    below = {"section": jnp.maximum(sec - 1, 0)}
    is_top = sec == sections - 1
    is_bottom = sec == 0

    loads = [
        pltpu.make_async_copy(src, dst, load_sem.at[i])
        for i, (src, dst) in enumerate(((wo_hbm, wo), (q_hbm, q), (k_hbm, k), (wv_hbm, wv)))
    ]
    for load in loads:
        load.start()

    barrier = pltpu.get_barrier_semaphore()
    for peer in (*dp_peers, *y_all):
        pl.semaphore_signal(barrier, inc=1, device_id=peer, device_id_type=MESH)

    @pl.when(jnp.logical_not(is_top))
    def _():
        pl.semaphore_signal(barrier, inc=1, device_id=above, device_id_type=MESH)

    @pl.when(jnp.logical_not(is_bottom))
    def _():
        pl.semaphore_signal(barrier, inc=1, device_id=below, device_id_type=MESH)

    linked = jnp.where(is_top, 0, 1) + jnp.where(is_bottom, 0, 1)
    pl.semaphore_wait(barrier, 6 + linked)

    def own_tokens(ref):
        return ref.at[:, pl.ds(pl.multiple_of(ten * part, part), part), :]

    def gathers(src, dst, send_sem, recv_sem):
        return [
            pltpu.make_async_remote_copy(
                src_ref=src,
                dst_ref=own_tokens(dst),
                send_sem=send_sem.at[i],
                recv_sem=recv_sem.at[i],
                device_id=peer,
                device_id_type=MESH,
            )
            for i, peer in enumerate(y_all)
        ]

    cot_copies = gathers(cot, cotg, ag_sem, agr_sem)
    inp_copies = gathers(inp, xg, xs_sem, xr_sem)

    @pl.when(is_top)
    def _():
        for copy in cot_copies:
            copy.start()
        cotg[:, pl.ds(pl.multiple_of(ten * part, part), part), :] = cot[...]

    heads = head_cols // HEAD_DIM
    loads[1].wait()
    loads[2].wait()
    rows_i = lax.broadcasted_iota(jnp.int32, (tokens, tokens), 0)
    cols_i = lax.broadcasted_iota(jnp.int32, (tokens, tokens), 1)
    allowed = (rows_i >= cols_i) & ((rows_i // seq) == (cols_i // seq))
    for h in range(heads):
        cols = slice(h * HEAD_DIM, (h + 1) * HEAD_DIM)
        q_head = q[:, :, cols].reshape(tokens, HEAD_DIM)
        k_head = k[:, :, cols].reshape(tokens, HEAD_DIM)
        scores = lax.dot_general(q_head, k_head, (((1,), (1,)), ((), ())), preferred_element_type=F32)
        scores = scores / jnp.sqrt(F32(HEAD_DIM))
        scores = jnp.where(allowed, scores, F32(-1e30))
        expo = jnp.exp(scores - jnp.max(scores, axis=-1, keepdims=True))
        att[h] = (expo / jnp.sum(expo, axis=-1, keepdims=True)).astype(BF16)

    n_ctx = head_cols // CTX_ROWS
    n_y = 4
    y_rows = width // n_y

    def forward(e):
        rows = pl.ds(e * y_rows, y_rows)
        return pltpu.make_async_remote_copy(
            src_ref=ufin.at[rows],
            dst_ref=u.at[rows],
            send_sem=fs_sem.at[e],
            recv_sem=fr_sem.at[e],
            device_id=below,
            device_id_type=MESH,
        )

    @pl.when(is_top)
    def _():
        for copy in cot_copies:
            copy.wait_recv()
        whole = cotg[...].reshape(tokens, width).astype(F32)
        u[...] = whole.T.astype(BF16)

    loads[0].wait()

    @pl.when(jnp.logical_not(is_top))
    def _():
        for e in range(n_y):
            forward(e).wait_recv()

    def ctx_copy(step, c):
        rows = pl.ds(c * CTX_ROWS, CTX_ROWS)
        return pltpu.make_async_remote_copy(
            src_ref=csend.at[step, rows],
            dst_ref=crecv.at[step, rows],
            send_sem=cs_sem.at[step, c],
            recv_sem=cr_sem.at[step, c],
            device_id=dp_peers[(c + step) % 3],
            device_id_type=MESH,
        )

    u_here = u[...]
    for c in range(n_ctx):
        rows = pl.ds(c * CTX_ROWS, CTX_ROWS)
        csend[0, rows] = jnp.dot(wo[rows], u_here, preferred_element_type=F32).astype(BF16)
        ctx_copy(0, c).start()

    for copy in inp_copies:
        copy.start()
    xg[:, pl.ds(pl.multiple_of(ten * part, part), part), :] = inp[...]

    for step in (0, 1):
        for c in range(n_ctx):
            rows = pl.ds(c * CTX_ROWS, CTX_ROWS)
            ctx_copy(step, c).wait_recv()
            csend[step + 1, rows] = (csend[step, rows].astype(F32) + crecv[step, rows].astype(F32)).astype(BF16)
            ctx_copy(step + 1, c).start()

    loads[3].wait()

    def y_copy(step, e):
        rows = pl.ds(e * y_rows, y_rows)
        return pltpu.make_async_remote_copy(
            src_ref=ysend.at[step, rows],
            dst_ref=yrecv.at[step, rows],
            send_sem=ys_sem.at[step, e],
            recv_sem=yr_sem.at[step, e],
            device_id=y_peers[(e + step) % 2],
            device_id_type=MESH,
        )

    for c in range(n_ctx):
        rows = pl.ds(c * CTX_ROWS, CTX_ROWS)
        ctx_copy(2, c).wait_recv()
        whole = (csend[2, rows].astype(F32) + crecv[2, rows].astype(F32)).astype(BF16)
        pieces = []
        for i in range(CTX_ROWS // HEAD_DIM):
            head = c * (CTX_ROWS // HEAD_DIM) + i
            pieces.append(
                jnp.dot(
                    whole[i * HEAD_DIM : (i + 1) * HEAD_DIM], att[head], preferred_element_type=F32
                ).astype(BF16)
            )
        value = jnp.concatenate(pieces, axis=0)
        vg_out[rows] = value
        if c < n_ctx - 1:
            term = jnp.dot(wv[:, rows], value, preferred_element_type=F32)
            acc[...] = term + (u[...].astype(F32) * F32(0.25) if c == 0 else acc[...])
        else:
            for e in range(n_y):
                y_part = pl.ds(e * y_rows, y_rows)
                term = jnp.dot(wv[y_part, rows], value, preferred_element_type=F32)
                ysend[0, y_part] = (acc[y_part] + term).astype(BF16)
                y_copy(0, e).start()

    for e in range(n_y):
        y_part = pl.ds(e * y_rows, y_rows)
        y_copy(0, e).wait_recv()
        ysend[1, y_part] = (ysend[0, y_part].astype(F32) + yrecv[0, y_part].astype(F32)).astype(BF16)
        y_copy(1, e).start()

    for e in range(n_y):
        y_part = pl.ds(e * y_rows, y_rows)
        y_copy(1, e).wait_recv()
        ufin[y_part] = (ysend[1, y_part].astype(F32) + yrecv[1, y_part].astype(F32)).astype(BF16)

        @pl.when(jnp.logical_not(is_bottom))
        def _():
            forward(e).start()

    turned[...] = ufin[...].astype(F32).T.astype(BF16)
    for m in range(micro):
        grad_out[m] = turned[pl.ds(pl.multiple_of(m * seq + ten * part, part), part), :]
    uin_out[...] = u[...]
    for copy in inp_copies:
        copy.wait_recv()
    xin_out[...] = xg[...]

    for copy in inp_copies:
        copy.wait_send()
    for step in range(3):
        for c in range(n_ctx):
            ctx_copy(step, c).wait_send()
    for step in range(2):
        for e in range(n_y):
            y_copy(step, e).wait_send()

    @pl.when(is_top)
    def _():
        for copy in cot_copies:
            copy.wait_send()

    @pl.when(jnp.logical_not(is_bottom))
    def _():
        for e in range(n_y):
            forward(e).wait_send()


def per_device(sections, cotangent, inputs, queries, keys, context, value_weight, out_weight):
    micro, part, width = cotangent.shape
    seq, head_cols = queries.shape[2], queries.shape[3]
    tokens = micro * seq
    heads = head_cols // HEAD_DIM
    n_ctx = head_cols // CTX_ROWS
    vmem = pl.BlockSpec(memory_space=pltpu.VMEM)
    anywhere = pl.BlockSpec(memory_space=pl.ANY)
    dma = pltpu.SemaphoreType.DMA
    grads, u_in, vg, x_in = pl.pallas_call(
        functools.partial(kernel, tokens, sections),
        out_shape=(
            jax.ShapeDtypeStruct((micro, part, width), BF16),
            jax.ShapeDtypeStruct((width, tokens), BF16),
            jax.ShapeDtypeStruct((head_cols, tokens), BF16),
            jax.ShapeDtypeStruct((micro, seq, width), BF16),
        ),
        in_specs=[vmem, vmem, anywhere, anywhere, anywhere, anywhere],
        out_specs=(vmem, vmem, vmem, vmem),
        scratch_shapes=[
            pltpu.VMEM((head_cols, width), BF16),
            pltpu.VMEM((width, head_cols), BF16),
            pltpu.VMEM((micro, seq, head_cols), BF16),
            pltpu.VMEM((micro, seq, head_cols), BF16),
            pltpu.VMEM((heads, tokens, tokens), BF16),
            pltpu.VMEM((micro, seq, width), BF16),
            pltpu.VMEM((micro, seq, width), BF16),
            pltpu.VMEM((width, tokens), BF16),
            pltpu.VMEM((3, head_cols, tokens), BF16),
            pltpu.VMEM((3, head_cols, tokens), BF16),
            pltpu.VMEM((width, tokens), F32),
            pltpu.VMEM((2, width, tokens), BF16),
            pltpu.VMEM((2, width, tokens), BF16),
            pltpu.VMEM((width, tokens), BF16),
            pltpu.VMEM((tokens, width), BF16),
            dma((4,)),
            dma((1,)),
            dma((3, n_ctx)),
            dma((3, n_ctx)),
            dma((2, 4)),
            dma((2, 4)),
            dma((4,)),
            dma((4,)),
            dma((3,)),
            dma((3,)),
            dma((3,)),
            dma((3,)),
        ],
        compiler_params=pltpu.CompilerParams(collective_id=0, has_side_effects=True),
    )(cotangent, inputs[0], queries[0], keys[0], out_weight[0], value_weight[0])
    context_flat = context[0].reshape(tokens, head_cols)
    out_grad = lax.dot_general(
        context_flat, u_in, (((0,), (1,)), ((), ())), preferred_element_type=F32
    ).astype(BF16)
    value_grad = lax.dot_general(
        x_in.reshape(tokens, width), vg, (((0,), (1,)), ((), ())), preferred_element_type=F32
    ).astype(BF16)
    return grads[None], value_grad[None], out_grad[None]


def solution(mesh):
    placed = (
        P(None, "tensor", "dp"),
        P("section", None, "tensor", "dp"),
        P("section", None, None, "tensor"),
        P("section", None, None, "tensor"),
        P("section", None, None, "tensor"),
        P("section", "dp", "tensor"),
        P("section", "tensor", "dp"),
    )
    return jax.shard_map(
        functools.partial(per_device, mesh.shape["section"]),
        mesh=mesh,
        in_specs=placed,
        out_specs=(
            P("section", None, "tensor", "dp"),
            P("section", "dp", "tensor"),
            P("section", "tensor", "dp"),
        ),
        check_vma=False,
    )
```
